32 devices in a mesh: group: 4 (over y, x), replica: 8 (over z, core).
Axes of the slice: x: 2, y: 2, z: 4, core: 2. Of those that a mesh axis runs over, the one named last changes fastest.
Arguments:
- activations: bfloat16 [4, 8, 290, 1024], P('group', 'replica'), may hold values from -40 to 40
- key_mask: int32 [4, 8, 290], P('group', 'replica'), may hold values from 0 to 1, as said below
- qkv_weight: bfloat16 [2, 1024, 3072], P(None, 'group'), may hold values from -4 to 4
- out_weight: bfloat16 [2, 1024, 1024], P(None, 'group'), may hold values from -0.5 to 0.5
- fc1_weight: bfloat16 [2, 1024, 4096], P(None, 'group'), may hold values from -0.1875 to 0.1875
- fc2_weight: bfloat16 [2, 4096, 1024], P(None, 'group'), may hold values from -0.09375 to 0.09375
- ln_gains: bfloat16 [2, 2, 1024], P(None, None, 'group'), may hold values from 0.5 to 1.5
- biases: bfloat16 [2, 6, 1024], P(None, None, 'group'), may hold values from -3 to 3
- fc1_bias: bfloat16 [2, 4096], P(None, 'group'), may hold values from -3 to 3
- cotangent: bfloat16 [4, 8, 290, 1024], P('group', 'replica'), may hold values from -6 to 6
Outputs:
- outputs: bfloat16 [4, 8, 290, 1024], P('group', 'replica')
- input_grad: bfloat16 [4, 8, 290, 1024], P('group', 'replica')
- grad_qkv: float32 [2, 1024, 3072], P(None, 'group')
- grad_out: float32 [2, 1024, 1024], P(None, 'group')
- grad_fc1: float32 [2, 1024, 4096], P(None, 'group')
- grad_fc2: float32 [2, 4096, 1024], P(None, 'group')
- grad_gains: float32 [2, 2, 1024], P(None, None, 'group')
- grad_biases: float32 [2, 6, 1024], P(None, None, 'group')
- grad_fc1_bias: float32 [2, 4096], P(None, 'group')
The draws below stay inside these ranges and needn't reach their ends.
Inputs may be any that keep to these rules, and one draw needn't show every extreme that they name: `key_mask`: each image has exactly 577 ones among its 580 positions, at places drawn at random.
All inputs are finite; a program needn't handle non-finite values.
Results may differ from the reference program's by a relative error of at most 0.017.
Values may be sent and summed in bfloat16 or wider, within the bound.
A program may use at most 320 MiB of HBM per device.

```python
import math
import jax
import jax.numpy as jnp
from jax import lax

D = 1024
HEAD = 64
FF = 4096
LAYERS = 2
SEQ = 580
VALID = 577
HALF = 290
SLOTS = 4
IMAGES_B = 8


def draw_activations(key, part):
    k_base, k_rows, k_cols = jax.random.split(key, 3)
    shape = (SLOTS, IMAGES_B, HALF, D)
    rows = jnp.exp(jax.random.uniform(k_rows, (SLOTS, IMAGES_B, HALF, 1), minval=math.log(0.3), maxval=math.log(3.0)))
    cols = jnp.exp(jax.random.uniform(k_cols, (D,), minval=math.log(0.5), maxval=math.log(2.0)))
    base = jax.random.normal(k_base, shape)
    return jnp.clip(base * rows * cols, -40.0, 40.0).astype(jnp.bfloat16)


def draw_key_mask(key, part):
    count = SLOTS // 2 * IMAGES_B
    keys = jax.random.split(key, count)
    orders = jax.vmap(lambda k: jax.random.permutation(k, SEQ))(keys)
    mask = (orders >= SEQ - VALID).astype(jnp.int32)
    mask = mask.reshape(SLOTS // 2, IMAGES_B, 2, HALF)
    return jnp.moveaxis(mask, 2, 1).reshape(SLOTS, IMAGES_B, HALF)


def draw_qkv_weight(key, part):
    shape = (LAYERS, D, 3 * D)
    base = jax.random.normal(key, shape)
    column = jnp.arange(3 * D)
    factor = jnp.where(column < 2 * D, 1.4142135, 1.0).astype(jnp.float32)
    return jnp.clip(base * factor * D ** (-0.5), -4.0, 4.0).astype(jnp.bfloat16)


def level_of(key, dims, cuts, smallest, largest):
    factor_of = 1.0
    for axis_at, parts in cuts:
        draws = jax.random.uniform(jax.random.fold_in(jax.random.fold_in(key, 6), axis_at), (parts,), jnp.float32, smallest / len(cuts), largest / len(cuts))
        factor_of = factor_of * jnp.repeat(jnp.exp(draws), dims[axis_at] // parts).reshape((-1,) + (1,) * (len(dims) - 1 - axis_at))
    return factor_of


def bell_draw(key, extent, deviation, limit, cuts=(), held_as=jnp.bfloat16):
    level = level_of(key, extent, cuts, -0.22, 0.18) if cuts else 1.0
    values = jax.random.normal(key, extent, jnp.float32) * deviation * level
    return jnp.minimum(jnp.maximum(values, -limit), limit).astype(held_as)


def setup_inputs(seed: int = 0) -> dict:
    streams_of = jax.random.split(jax.random.key(seed), 11)
    return {
        "activations": draw_activations(jax.random.fold_in(streams_of[10], 71), 0),
        "key_mask": draw_key_mask(jax.random.fold_in(streams_of[10], 71), 0),
        "qkv_weight": draw_qkv_weight(jax.random.fold_in(streams_of[10], 71), 0),
        "out_weight": bell_draw(streams_of[3], (LAYERS, D, D), (D // 8) ** -0.5, 0.5, ((1, 4),)),
        "fc1_weight": bell_draw(streams_of[4], (LAYERS, D, FF), D ** -0.5, 0.1875, ((1, 4),)),
        "fc2_weight": bell_draw(streams_of[5], (LAYERS, FF, D), FF ** -0.5, 0.09375, ((1, 4),)),
        "ln_gains": jnp.clip(1.0 + 0.1 * jax.random.normal(streams_of[6], (LAYERS, 2, D), jnp.float32), 0.5, 1.5).astype(jnp.bfloat16),
        "biases": bell_draw(streams_of[7], (LAYERS, 6, D), 0.5, 3.0, ((2, 4),)),
        "fc1_bias": bell_draw(streams_of[8], (LAYERS, FF), 0.5, 3.0, ((1, 4),)),
        "cotangent": bell_draw(streams_of[9], (SLOTS, IMAGES_B, HALF, D), 1.0, 6.0, ((0, 4), (1, 8))),
    }


@jax.custom_vjp
def low(v):
    return lax.optimization_barrier(v.astype(jnp.bfloat16)).astype(jnp.float32)

@jax.custom_vjp
def low_back(v):
    return v

def low_keep(v):
    return (low(v), None)

def low_pass(kept, grad):
    return (grad,)

def back_keep(v):
    return (v, None)

def back_low(kept, grad):
    return (low(grad),)
low.defvjp(low_keep, low_pass)
low_back.defvjp(back_keep, back_low)
HIGH = lax.Precision.HIGHEST
EPS = 1e-06

def layer_norm(v, gain, shift):
    mean = lax.optimization_barrier(jnp.mean(v, axis=-1, keepdims=True))
    centred = v - mean
    var = lax.optimization_barrier(jnp.mean(centred * centred, axis=-1, keepdims=True))
    return centred * lax.rsqrt(var + EPS) * gain + shift

def block(stream, valid, weights):
    wqkv, wout, wfc1, wfc2, gains, shifts, fc1b = weights
    images, seq, width = stream.shape
    heads = width // HEAD
    normed = low(layer_norm(stream, gains[0], shifts[0]))
    mixed = jnp.einsum('isd,de->ise', normed, wqkv, precision=HIGH)
    query = low(low_back((mixed[..., :width] + shifts[1]) * HEAD ** (-0.5)))
    key = low(low_back(mixed[..., width:2 * width]))
    value = low(low_back(mixed[..., 2 * width:] + shifts[2]))
    query = query.reshape(images, seq, heads, HEAD)
    key = key.reshape(images, seq, heads, HEAD)
    value = value.reshape(images, seq, heads, HEAD)
    scores = low_back(jnp.einsum('iqhd,ikhd->ihqk', query, key, precision=HIGH))
    scores = jnp.where(valid[:, None, None, :] > 0, scores, -1e+30)
    attn = low(jax.nn.softmax(scores, axis=-1))
    context = jnp.einsum('ihqk,ikhd->iqhd', attn, value, precision=HIGH).reshape(images, seq, width)
    context = low(low_back(context))
    branch = low_back(jnp.einsum('isd,de->ise', context, wout, precision=HIGH) + shifts[3])
    middle = stream + branch
    normed_b = low(layer_norm(middle, gains[1], shifts[4]))
    pre = low_back(jnp.einsum('isd,df->isf', normed_b, wfc1, precision=HIGH) + fc1b)
    act = low(jax.nn.gelu(pre, approximate=False))
    out = low_back(jnp.einsum('isf,fd->isd', act, wfc2, precision=HIGH) + shifts[5])
    return middle + out

def arrange(v):
    rest = v.shape[3:]
    v = v.reshape((SLOTS // 2, 2, IMAGES_B, HALF) + rest)
    v = jnp.moveaxis(v, 1, 2)
    return v.reshape((SLOTS // 2 * IMAGES_B, SEQ) + rest)

def restore(v):
    rest = v.shape[2:]
    v = v.reshape((SLOTS // 2, IMAGES_B, 2, HALF) + rest)
    v = jnp.moveaxis(v, 2, 1)
    return v.reshape((SLOTS, IMAGES_B, HALF) + rest)

def reference(activations, key_mask, qkv_weight, out_weight, fc1_weight, fc2_weight, ln_gains, biases, fc1_bias, cotangent):
    stream = arrange(activations.astype(jnp.float32))
    valid = arrange(key_mask)
    cotan = arrange(cotangent.astype(jnp.float32))
    params = tuple((w.astype(jnp.float32) for w in (qkv_weight, out_weight, fc1_weight, fc2_weight, ln_gains, biases, fc1_bias)))
    width = stream.shape[-1]

    def forward(state, mask_rows, weights):
        for layer in range(LAYERS):
            state = block(state, mask_rows, tuple((w[layer] for w in weights)))
        return state

    def step(totals, piece):
        state, mask_rows, cot_rows = piece
        result, pull = jax.vjp(lambda s_, w_: forward(s_, mask_rows, w_), state, params)
        d_state, d_params = pull(cot_rows)
        totals = jax.tree.map(lambda a, b: a + b, totals, d_params)
        return (totals, (result, d_state))
    zeros = jax.tree.map(jnp.zeros_like, params)
    pieces = (stream.reshape(-1, 4, SEQ, width), valid.reshape(-1, 4, SEQ), cotan.reshape(-1, 4, SEQ, width))
    totals, (results, d_inputs) = lax.scan(step, zeros, pieces)
    outputs = restore(results.reshape(-1, SEQ, width)).astype(jnp.bfloat16)
    input_grad = restore(d_inputs.reshape(-1, SEQ, width)).astype(jnp.bfloat16)
    return (outputs, input_grad, totals[0], totals[1], totals[2], totals[3], totals[4], totals[5], totals[6])
```

```python
import functools

import jax
import jax.numpy as jnp
from jax import lax
from jax.experimental import pallas as pl
from jax.experimental.pallas import tpu as pltpu
from jax.sharding import PartitionSpec as P

HEAD = 64
EPS = 1e-06
F32 = jnp.float32
BF16 = jnp.bfloat16
TILE = 256
ROWS = 16
VMEM = pl.BlockSpec(memory_space=pltpu.VMEM)
SMEM = pl.BlockSpec(memory_space=pltpu.SMEM)
ANY = pl.BlockSpec(memory_space=pl.ANY)


def swap(value, axis, mask):
    pairs = [(source, source ^ mask) for source in range(lax.axis_size(axis))]
    return lax.ppermute(value, axis, pairs)


def dot(a, b):
    return lax.dot_general(a, b, (((1,), (0,)), ((), ())), preferred_element_type=F32)


def dot_nt(a, b):
    return lax.dot_general(a, b, (((1,), (1,)), ((), ())), preferred_element_type=F32)


def dot_tn(a, b):
    return lax.dot_general(a, b, (((0,), (0,)), ((), ())), preferred_element_type=F32)


def shape(dims, dtype=BF16):
    return jax.ShapeDtypeStruct(dims, dtype)


def call(body, name, ins, outs, scratch=(), flops=0, **kwargs):
    size = sum(a.size * a.dtype.itemsize for _, a in ins)
    size += sum(s.size * s.dtype.itemsize for _, s in outs)
    return pl.pallas_call(
        functools.partial(body, **kwargs),
        name=name,
        in_specs=[s for s, _ in ins],
        out_specs=[s for s, _ in outs],
        out_shape=[s for _, s in outs],
        scratch_shapes=list(scratch),
        cost_estimate=pl.CostEstimate(flops=flops, bytes_accessed=size, transcendentals=0),
        compiler_params=pltpu.CompilerParams(vmem_limit_bytes=56 * 2**20),
    )(*[a for _, a in ins])


def loop(count, body):
    lax.fori_loop(0, count, lambda i, _: (body(i), None)[1], None)


def lanes(i, size=TILE):
    return pl.ds(pl.multiple_of(i * size, size), size)


def chunk(i):
    return pl.ds(pl.multiple_of(i * ROWS, ROWS), ROWS)


def pack_body(pos, *refs, layer, parts, halves):
    n = len(parts) + halves
    ws, outs, sem = refs[:n], refs[n:-1], refs[-1]
    x, core = pos[0], pos[2]
    copies, at = [], 0
    for w, part in zip(ws[: len(parts)], parts):
        h, cols = outs[at].shape
        f = w.shape[2] // part[0]
        rows = pl.ds(pl.multiple_of(core * h, h), h)
        for to, of in ((outs[at], 1 - x), (outs[at + 1], x)):
            for i in range(cols // f):
                source = w.at[layer, rows, pl.ds(pl.multiple_of((i * 2 + of) * f, f), f)]
                copies.append((source, to.at[:, pl.ds(i * f, f)]))
        at += 2
    for w in ws[len(parts) :]:
        h = outs[at].shape[0]
        copies.append((w.at[layer, pl.ds(pl.multiple_of(core * h, h), h)], outs[at]))
        at += 1
    run(copies, sem)


def run(copies, sem, at=0):
    started = [pltpu.make_async_copy(s, d, sem.at[at + i]) for i, (s, d) in enumerate(copies)]
    for c in started:
        c.start()
    for c in started:
        c.wait()


def column_copies(pos, w, pieces, to, layer, group, parts):
    x, y, core = pos[0], pos[1], pos[2]
    dg = w.shape[1]
    h = dg // 2
    f = w.shape[2] // (parts * group)
    copies = []
    mine = pl.ds(pl.multiple_of((y * 2 + x) * dg, dg), dg)
    for i in range(parts * group // 2):
        source = w.at[layer, :, pl.ds(pl.multiple_of((i * 2 + x) * f, f), f)]
        copies.append((source, to.at[mine, pl.ds(i * f, f)]))
    for (yi, xi, ci), piece in pieces:
        row = ((y ^ yi) * 2 + (x ^ xi)) * dg + (core ^ ci) * h
        copies.append((piece, to.at[pl.ds(pl.multiple_of(row, h), h)]))
    return copies


def row_copies(pos, w, pieces, to, layer):
    y, core = pos[1], pos[2]
    r = w.shape[1]
    h = r // 2
    copies = [(w.at[layer], to.at[pl.ds(pl.multiple_of(y * r, r), r)])]
    for (k, ci), piece in pieces:
        row = (y ^ k) * r + (core ^ ci) * h
        copies.append((piece, to.at[pl.ds(pl.multiple_of(row, h), h)]))
    return copies


def layer_norm_rows(v, gain, shift):
    mean = jnp.mean(v, axis=-1, keepdims=True)
    centred = v - mean
    var = jnp.mean(centred * centred, axis=-1, keepdims=True)
    return (centred * lax.rsqrt(var + EPS) * gain + shift).astype(BF16)


def first_norm_body(act, gain, shift, stream, ln):
    n = act.shape[0]
    full = n // ROWS

    def step(i):
        v = act[chunk(i), :].astype(F32)
        stream[chunk(i), :] = v
        ln[chunk(i), :] = layer_norm_rows(v, gain[...], shift[...])

    loop(full, step)
    if n % ROWS:
        v = act[full * ROWS :, :].astype(F32)
        v = jnp.concatenate([v, jnp.zeros((ROWS - n % ROWS, v.shape[1]), F32)], axis=0)
        stream[full * ROWS :, :] = v
        ln[full * ROWS :, :] = layer_norm_rows(v, gain[...], shift[...])


def norm_body(base, part, got, bias, gain, shift, stream, ln):
    def step(i):
        v = base[chunk(i), :] + (part[chunk(i), :] + got[chunk(i), :].astype(F32)) + bias[...]
        stream[chunk(i), :] = v
        ln[chunk(i), :] = layer_norm_rows(v, gain[...], shift[...])

    loop(base.shape[0] // ROWS, step)


def last_body(base, part, got, bias, out):
    n = out.shape[0]
    full = n // ROWS

    def value(i):
        v = base[chunk(i), :] + (part[chunk(i), :] + got[chunk(i), :].astype(F32)) + bias[...]
        return v.astype(BF16)

    def step(i):
        out[chunk(i), :] = value(i)

    loop(full, step)
    if n % ROWS:
        out[full * ROWS :, :] = value(full)[: n % ROWS]


def first_grad_body(cot, grad, g, sums):
    n = cot.shape[0]
    full = n // ROWS
    sums[...] = jnp.zeros_like(sums)

    def put(at, v):
        grad[at, :] = v.astype(F32)
        g[at, :] = v
        sums[...] += jnp.sum(v.astype(F32), axis=0, keepdims=True)

    def step(i):
        put(chunk(i), cot[chunk(i), :])

    loop(full, step)
    if n % ROWS:
        v = cot[full * ROWS :, :]
        v = jnp.concatenate([v, jnp.zeros((ROWS - n % ROWS, v.shape[1]), BF16)], axis=0)
        put(pl.ds(full * ROWS, ROWS), v)


def norm_back_body(part, got, base, gain, before, after, g, sums):
    sums[...] = jnp.zeros_like(sums)
    n = g.shape[0]

    def step(i):
        d = part[chunk(i), :] + got[chunk(i), :].astype(F32)
        v = base[chunk(i), :]
        mean = jnp.mean(v, axis=-1, keepdims=True)
        centred = v - mean
        var = jnp.mean(centred * centred, axis=-1, keepdims=True)
        inv = lax.rsqrt(var + EPS)
        xhat = centred * inv
        e = d * gain[...]
        m1 = jnp.mean(e, axis=-1, keepdims=True)
        m2 = jnp.mean(e * xhat, axis=-1, keepdims=True)
        r = before[chunk(i), :] + (e - m1 - xhat * m2) * inv
        low = r.astype(BF16)
        after[chunk(i), :] = r
        g[chunk(i), :] = low
        sums[0:1, :] += jnp.sum(d * xhat, axis=0, keepdims=True)
        sums[1:2, :] += jnp.sum(d, axis=0, keepdims=True)
        sums[2:3, :] += jnp.sum(low.astype(F32), axis=0, keepdims=True)

    loop(n // ROWS, step)


def project(ln, w, bias, out, width):
    def step(i):
        v = dot(ln[...], w[:, lanes(i)]) + bias[:, lanes(i)]
        factor = jnp.where(i * TILE < width, HEAD ** (-0.5), 1.0)
        out[:, lanes(i)] = (v * factor).astype(BF16)

    loop(out.shape[1] // TILE, step)


def qkv_body(pos, ln, bias, w_all, *refs, layer, group, keys):
    pieces, (out, w, sem) = refs[:-3], refs[-3:]
    run(column_copies(pos, w_all, list(zip(keys, pieces)), w, layer, group, 3), sem)
    project(ln, w, bias, out, out.shape[1] // 3)


def attend(q, kv, mask, probs, ctx, width):
    first = lax.broadcasted_iota(jnp.int32, (1, 2 * HEAD), 1) < HEAD
    for hp in range(width // (2 * HEAD)):
        cols = slice(hp * 2 * HEAD, (hp + 1) * 2 * HEAD)
        q2 = q[:, cols]
        k2 = kv[:, cols]
        v2 = kv[:, slice(width + cols.start, width + cols.stop)]
        outs = []
        for e in range(2):
            keep = first if e == 0 else jnp.logical_not(first)
            s = dot_nt(jnp.where(keep, q2, jnp.zeros_like(q2)), k2) + mask[...]
            top = jnp.max(s, axis=-1, keepdims=True)
            ex = jnp.exp(s - top)
            p = (ex * (1.0 / jnp.sum(ex, axis=-1, keepdims=True))).astype(BF16)
            probs[hp * 2 + e] = p
            outs.append(dot(p, v2))
        ctx[:, cols] = jnp.where(first, outs[0], outs[1]).astype(BF16)


def join(own, other, kv, width):
    n = own.shape[0]
    kv[0:n, :] = own[:, width:]
    kv[n:, :] = other[:, width:]


def matmul(a, w, out):
    def step(i):
        out[:, lanes(i)] = dot(a[...], w[:, lanes(i)]).astype(out.dtype)

    loop(out.shape[1] // TILE, step)


def matmul_nt(a, w, out):
    def step(i):
        out[:, lanes(i)] = dot_nt(a[...], w[lanes(i), :]).astype(out.dtype)

    loop(out.shape[1] // TILE, step)


def attend_other_body(pos, ln, w, bias, own, mask, wout_all, *refs, layer, keys):
    pieces, (qkv, probs, ctx, partial, wout, kv, sem) = refs[:-7], refs[-7:]
    width = ctx.shape[1]
    copies = row_copies(pos, wout_all, list(zip(keys, pieces)), wout, layer)
    copies = [pltpu.make_async_copy(s, d, sem.at[i]) for i, (s, d) in enumerate(copies)]
    for c in copies:
        c.start()
    project(ln, w, bias, qkv, width)
    join(own, qkv, kv, width)
    attend(qkv.at[:, 0:width], kv, mask, probs, ctx, width)
    for c in copies:
        c.wait()
    matmul(ctx, wout, partial)


def attend_own_body(own, other, mask, wout, probs, ctx, partial, kv):
    width = ctx.shape[1]
    join(own, other, kv, width)
    attend(own.at[:, 0:width], kv, mask, probs, ctx, width)
    matmul(ctx, wout, partial)


def hidden(mlp, w1, bias, act, slope):
    def step(i):
        v = dot(mlp[...], w1[:, lanes(i)]) + bias[:, lanes(i)]
        cdf = 0.5 * (1.0 + lax.erf(v * (0.5**0.5)))
        pdf = jnp.exp(-0.5 * v * v) * 0.3989422804014327
        act[:, lanes(i)] = (v * cdf).astype(BF16)
        slope[:, lanes(i)] = (cdf + v * pdf).astype(BF16)

    loop(act.shape[1] // TILE, step)


def mlp_own_body(pos, mlp, bias, w1_all, w2_all, *refs, layer, group, keys1, keys2):
    pieces, (act, slope, partial, w1, w2, sem) = refs[:-6], refs[-6:]
    one = column_copies(
        pos, w1_all, list(zip(keys1, pieces[: len(keys1)])), w1, layer, group, 1
    )
    two = row_copies(pos, w2_all, list(zip(keys2, pieces[len(keys1) :])), w2, layer)
    copies = [pltpu.make_async_copy(s, d, sem.at[i]) for i, (s, d) in enumerate(one + two)]
    for c in copies:
        c.start()
    for c in copies[: len(one)]:
        c.wait()
    hidden(mlp, w1, bias, act, slope)
    for c in copies[len(one) :]:
        c.wait()
    matmul(act, w2, partial)


def mlp_other_body(mlp, bias, w1, w2, act, slope, partial):
    hidden(mlp, w1, bias, act, slope)
    matmul(act, w2, partial)


def mlp_back_body(g, slope, w2, w1, d_pre, d_mlp, sums):
    def step(i):
        v = dot_nt(g[...], w2[lanes(i), :]) * slope[:, lanes(i)].astype(F32)
        v = v.astype(BF16)
        d_pre[:, lanes(i)] = v
        sums[:, lanes(i)] = jnp.sum(v.astype(F32), axis=0, keepdims=True)

    loop(d_pre.shape[1] // TILE, step)
    matmul_nt(d_pre, w1, d_mlp)


def load_pairs(pairs, sem):
    copies = []
    for i, ((own, other), buffer) in enumerate(pairs):
        n = own.shape[0]
        copies.append(
            (
                pltpu.make_async_copy(own, buffer.at[0:n], sem.at[2 * i]),
                pltpu.make_async_copy(other, buffer.at[n:], sem.at[2 * i + 1]),
            )
        )
    for pair in copies:
        for c in pair:
            c.start()

    def wait(i):
        for c in copies[i]:
            c.wait()

    return wait


def column_grads(lhs, rhs, keep, send, core, parts):
    cols = keep.shape[1] // parts
    per = cols // TILE

    def step(i):
        p, t = i // per, i % per
        for to, half in ((keep, core), (send, 1 - core)):
            at = pl.multiple_of(p * 2 * cols + half * cols + t * TILE, TILE)
            to[:, lanes(i)] = dot_tn(lhs[...], rhs[:, pl.ds(at, TILE)]).astype(BF16)

    loop(parts * per, step)


def row_grads(lhs, rhs, keep, send, core):
    half = keep.shape[1]

    def step(i):
        for to, of in ((keep, core), (send, 1 - core)):
            at = pl.multiple_of(of * half + i * TILE, TILE)
            to[:, lanes(i)] = dot_tn(lhs[...], rhs[:, pl.ds(at, TILE)]).astype(BF16)

    loop(half // TILE, step)


def mlp_grads_body(pos, *refs):
    ins, (k1, s1, k2, s2, mlp, d_pre, act, g, sem) = refs[:8], refs[8:]
    core = pos[2]
    pairs = [(ins[2 * i : 2 * i + 2], b) for i, b in enumerate((act, g, mlp, d_pre))]
    wait = load_pairs(pairs, sem)
    wait(0), wait(1)
    row_grads(act, g, k2, s2, core)
    wait(2), wait(3)
    column_grads(mlp, d_pre, k1, s1, core, 1)


def attend_back(ga, wout, q, kv, probs, d_ctx, d_q, d_kv, width):
    matmul_nt(ga, wout, d_ctx)
    first = lax.broadcasted_iota(jnp.int32, (1, 2 * HEAD), 1) < HEAD
    for hp in range(width // (2 * HEAD)):
        cols = slice(hp * 2 * HEAD, (hp + 1) * 2 * HEAD)
        vcols = slice(width + cols.start, width + cols.stop)
        q2, k2, v2, c2 = q[:, cols], kv[:, cols], kv[:, vcols], d_ctx[:, cols]
        dq, dk, dv = [], [], []
        for e in range(2):
            keep = first if e == 0 else jnp.logical_not(first)
            p = probs[hp * 2 + e]
            d = dot_nt(jnp.where(keep, c2, jnp.zeros_like(c2)), v2)
            pf = p.astype(F32)
            delta = jnp.sum(pf * d, axis=-1, keepdims=True)
            ds = (pf * (d - delta)).astype(BF16)
            dq.append(dot(ds, k2))
            dk.append(dot_tn(ds, q2))
            dv.append(dot_tn(p, c2))
        d_q[:, cols] = (
            jnp.where(first, dq[0], dq[1]).astype(BF16).astype(F32) * HEAD ** (-0.5)
        ).astype(BF16)
        d_kv[:, cols] += jnp.where(first, dk[0], dk[1])
        d_kv[:, vcols] += jnp.where(first, dv[0], dv[1])


def attend_back_own_body(ga, wout, own, other, probs, d_q, d_kv, kv, d_ctx):
    width = d_q.shape[1]
    join(own, other, kv, width)
    d_kv[...] = jnp.zeros_like(d_kv)
    attend_back(ga, wout, own.at[:, 0:width], kv, probs, d_ctx, d_q, d_kv, width)


def attend_back_other_body(
    ga, wout, own, other, probs, d_q, d_kv_in, w, mixed_o, mixed_t, d_ln, sums, kv, d_ctx, d_kv, d_qt
):
    width = d_q.shape[1]
    n = own.shape[0]
    join(own, other, kv, width)
    d_kv[...] = d_kv_in[...]
    attend_back(ga, wout, other.at[:, 0:width], kv, probs, d_ctx, d_qt, d_kv, width)
    mixed_o[:, 0:width] = d_q[...]
    mixed_t[:, 0:width] = d_qt[...]
    mixed_o[:, width:] = d_kv[0:n, :].astype(BF16)
    mixed_t[:, width:] = d_kv[n:, :].astype(BF16)
    matmul_nt(mixed_t, w, d_ln)
    for at in range(0, 3 * width, width):
        cols = slice(at, at + width)
        sums[:, cols] = jnp.sum(mixed_o[:, cols].astype(F32), axis=0, keepdims=True) + jnp.sum(
            mixed_t[:, cols].astype(F32), axis=0, keepdims=True
        )


def attend_grads_body(pos, mixed, w, *refs):
    ins, (d_ln, k1, s1, k2, s2, ctx, ga, ln, d_mixed, sem) = refs[:8], refs[8:]
    core = pos[2]
    pairs = [(ins[2 * i : 2 * i + 2], b) for i, b in enumerate((ctx, ga, ln, d_mixed))]
    wait = load_pairs(pairs, sem)
    matmul_nt(mixed, w, d_ln)
    wait(0), wait(1)
    row_grads(ctx, ga, k2, s2, core)
    wait(2), wait(3)
    column_grads(ln, d_mixed, k1, s1, core, 3)


def place_body(pos, own, other, out, *, parts, group):
    x, core = pos[0], pos[2]
    dg, total = out.shape
    f = total // (parts * group)
    per = group // 4
    for v, c in ((own, core), (other, 1 - core)):
        for xi in range(2):
            for p in range(parts):
                for j in range(per):
                    at = ((p * (group // 2) + c * per + j) * 2 + (x ^ xi)) * f
                    out[:, pl.ds(pl.multiple_of(at, f), f)] = v[
                        xi * dg : (xi + 1) * dg, (p * per + j) * f : (p * per + j + 1) * f
                    ].astype(F32)


def place_rows_body(pos, own, other, out):
    core = pos[2]
    half = own.shape[1]
    for v, c in ((own, core), (other, 1 - core)):
        out[:, pl.ds(pl.multiple_of(c * half, half), half)] = v[...].astype(F32)


def shards(
    activations,
    key_mask,
    qkv_weight,
    out_weight,
    fc1_weight,
    fc2_weight,
    ln_gains,
    biases,
    fc1_bias,
    cotangent,
):
    layers = qkv_weight.shape[0]
    n = activations.shape[2]
    npad = -(-n // ROWS) * ROWS
    width = activations.shape[3]
    half = width // 2
    group, replica = lax.axis_size("group"), lax.axis_size("replica")
    ys, zs = group // 2, replica // 2
    dg = width // group
    h = dg // 2
    ffg = fc2_weight.shape[1]
    ff = ffg * ys
    many = ffg // dg
    heads = half // HEAD
    me, rep = lax.axis_index("group"), lax.axis_index("replica")
    x, y = me % 2, me // 2
    core, z = rep % 2, rep // 2
    pos = jnp.stack([x, y, core, z]).astype(jnp.int32)

    def over_x(v):
        return swap(v, "group", 1)

    def over_y(v, k):
        return swap(v, "group", 2 * k)

    def over_core(v):
        return swap(v, "replica", 1)

    def over_z(v, k):
        return swap(v, "replica", 2 * k)

    sems = pltpu.SemaphoreType.DMA

    def pack(layer, columns, rows):
        ins = [(SMEM, pos)] + [(ANY, w) for w, _ in columns] + [(ANY, w) for w in rows]
        outs = []
        for w, _ in columns:
            outs += [(VMEM, shape((h, w.shape[2] // 2)))] * 2
        outs += [(VMEM, shape((w.shape[1] // 2, width))) for w in rows]
        parts = [(p * group,) for _, p in columns]
        return call(
            pack_body,
            "pack",
            ins,
            outs,
            [sems((64,))],
            layer=layer,
            parts=parts,
            halves=len(rows),
        )

    def spread_columns(theirs, ours):
        got = over_x(theirs)
        pieces = {(0, 1, 0): got}
        for k in range(1, ys):
            pieces[k, 0, 0] = over_y(ours, k)
            pieces[k, 1, 0] = over_y(got, k)
        for (yi, xi, _), v in list(pieces.items()):
            pieces[yi, xi, 1] = over_core(v)
        return pieces

    def spread_rows(v):
        pieces = {}
        for k in range(1, ys):
            pieces[k, 0] = over_y(v, k)
            pieces[k, 1] = over_core(pieces[k, 0])
        return pieces

    fetched = []
    for layer in range(layers):
        qx, qy, ro = pack(layer, [(qkv_weight, 3)], [out_weight])
        fx, fy, rf = pack(layer, [(fc1_weight, 1)], [fc2_weight])
        fetched.append(
            (spread_columns(qx, qy), spread_rows(ro), spread_columns(fx, fy), spread_rows(rf))
        )

    small = jnp.concatenate(
        [
            ln_gains.reshape(layers * 2, dg),
            biases.reshape(layers * 6, dg),
            fc1_bias.reshape(layers * many, dg),
        ],
        axis=0,
    )
    small = lax.all_gather(small, "group", axis=0)
    rows_of = jnp.moveaxis(small[:, : layers * 8], 0, 1).reshape(layers * 8, width).astype(F32)
    mine = lax.dynamic_index_in_dim(small.reshape(ys, 2, -1, dg), x, 1, keepdims=False).astype(F32)

    def gain(layer, i):
        return rows_of[layer * 2 + i][None]

    def shift(layer, i):
        return rows_of[layers * 2 + layer * 6 + i][None]

    def head_shift(layer):
        at = layers * 2 + layer * 6
        q, v = mine[:, at + 1].reshape(1, half), mine[:, at + 2].reshape(1, half)
        return jnp.concatenate([q, jnp.zeros_like(q), v], axis=1)

    def fc1_shift(layer):
        at = layers * 8 + layer * many
        return mine[:, at : at + many].reshape(1, ff)

    mask_o = jnp.where(key_mask.reshape(n) > 0, 0.0, -1e30).astype(BF16)
    mask_o = jnp.pad(mask_o, (0, npad - n), constant_values=-1e30)
    mask = jnp.concatenate([mask_o, over_x(mask_o)]).astype(F32)[None]

    tok = shape((npad, width))
    tok32 = shape((npad, width), F32)
    qkv_s = shape((npad, 3 * half))
    probs_s = shape((heads, npad, 2 * npad))
    ctx_s = shape((npad, half))
    hid = shape((npad, ff))
    kv_v = pltpu.VMEM((2 * npad, 2 * half), BF16)
    gemm = 2 * npad * width

    saved = []
    stream, ln_o = call(
        first_norm_body,
        "norm",
        [(VMEM, activations.reshape(n, width)), (VMEM, gain(0, 0)), (VMEM, shift(0, 0))],
        [(VMEM, tok32), (VMEM, tok)],
    )
    for layer in range(layers):
        pq, po, p1, p2 = fetched[layer]
        ln_t = over_x(ln_o)
        qkv_o, wqkv = call(
            qkv_body,
            "qkv",
            [(SMEM, pos), (VMEM, ln_o), (VMEM, head_shift(layer)), (ANY, qkv_weight)]
            + [(ANY, v) for v in pq.values()],
            [(VMEM, qkv_s), (VMEM, shape((width, 3 * half)))],
            [sems((64,))],
            gemm * 3 * half,
            layer=layer,
            group=group,
            keys=list(pq),
        )
        qkv_t, probs_t, ctx_t, send, wout = call(
            attend_other_body,
            "attend_other",
            [
                (SMEM, pos),
                (VMEM, ln_t),
                (VMEM, wqkv),
                (VMEM, head_shift(layer)),
                (VMEM, qkv_o),
                (VMEM, mask),
                (ANY, out_weight),
            ]
            + [(ANY, v) for v in po.values()],
            [(VMEM, s) for s in (qkv_s, probs_s, ctx_s, tok, shape((half, width)))],
            [kv_v, sems((16,))],
            gemm * 5 * half,
            layer=layer,
            keys=list(po),
        )
        got = over_x(send)
        probs_o, ctx_o, part = call(
            attend_own_body,
            "attend_own",
            [(VMEM, v) for v in (qkv_o, qkv_t, mask, wout)],
            [(VMEM, s) for s in (probs_s, ctx_s, tok32)],
            [kv_v],
            gemm * 3 * half,
        )
        middle, mlp_o = call(
            norm_body,
            "norm",
            [
                (VMEM, v)
                for v in (stream, part, got, shift(layer, 3), gain(layer, 1), shift(layer, 4))
            ],
            [(VMEM, tok32), (VMEM, tok)],
        )
        mlp_t = over_x(mlp_o)
        act_o, slope_o, part, w1, w2 = call(
            mlp_own_body,
            "mlp_own",
            [
                (SMEM, pos),
                (VMEM, mlp_o),
                (VMEM, fc1_shift(layer)),
                (ANY, fc1_weight),
                (ANY, fc2_weight),
            ]
            + [(ANY, v) for v in p1.values()]
            + [(ANY, v) for v in p2.values()],
            [(VMEM, s) for s in (hid, hid, tok32, shape((width, ff)), shape((ff, width)))],
            [sems((64,))],
            gemm * 2 * ff,
            layer=layer,
            group=group,
            keys1=list(p1),
            keys2=list(p2),
        )
        act_t, slope_t, send = call(
            mlp_other_body,
            "mlp_other",
            [(VMEM, v) for v in (mlp_t, fc1_shift(layer), w1, w2)],
            [(VMEM, s) for s in (hid, hid, tok)],
            (),
            gemm * 2 * ff,
        )
        got = over_x(send)
        saved.append(
            dict(
                stream=stream,
                middle=middle,
                ln=(ln_o, ln_t),
                qkv=(qkv_o, qkv_t),
                probs=(probs_o, probs_t),
                ctx=(ctx_o, ctx_t),
                mlp=(mlp_o, mlp_t),
                act=(act_o, act_t),
                slope=(slope_o, slope_t),
                w=(wqkv, wout, w1, w2),
            )
        )
        if layer + 1 < layers:
            stream, ln_o = call(
                norm_body,
                "norm",
                [
                    (VMEM, v)
                    for v in (
                        middle,
                        part,
                        got,
                        shift(layer, 5),
                        gain(layer + 1, 0),
                        shift(layer + 1, 0),
                    )
                ],
                [(VMEM, tok32), (VMEM, tok)],
            )
        else:
            outputs = call(
                last_body,
                "last",
                [(VMEM, v) for v in (middle, part, got, shift(layer, 5))],
                [(VMEM, shape((n, width)))],
            )[0]

    def add(a, b):
        return (a.astype(F32) + b.astype(F32)).astype(BF16)

    def all_z(v):
        m = v.shape[0] // 2
        bit = z % 2
        keep = lax.dynamic_slice(v, (bit * m, 0), (m, v.shape[1]))
        send = lax.dynamic_slice(v, ((1 - bit) * m, 0), (m, v.shape[1]))
        keep = add(keep, over_z(send, 1))
        k = 2
        while k < zs:
            keep = add(keep, over_z(keep, k))
            k *= 2
        other = over_z(keep, 1)
        return jnp.where(
            bit == 0,
            jnp.concatenate([keep, other], axis=0),
            jnp.concatenate([other, keep], axis=0),
        )

    def pick_rows(v, at, size):
        return lax.dynamic_slice(v, (at * size, 0), (size, v.shape[1]))

    def reduce_y(keep, send, size):
        total = add(keep, over_core(send))
        own = pick_rows(total, y, size)
        for k in range(1, ys):
            own = add(own, over_y(pick_rows(total, y ^ k, size), k))
        return own

    def finish_columns(keep, send, parts):
        own = reduce_y(keep, send, 2 * dg)
        got = over_x(pick_rows(own, 1 - x, dg))
        own = all_z(jnp.concatenate([pick_rows(own, x, dg), got], axis=0))
        return call(
            place_body,
            "place",
            [(SMEM, pos), (VMEM, own), (VMEM, over_core(own))],
            [(VMEM, shape((dg, keep.shape[1] * 4), F32))],
            parts=parts,
            group=group,
        )[0]

    def finish_rows(keep, send, size):
        own = all_z(reduce_y(keep, send, size))
        return call(
            place_rows_body,
            "place_rows",
            [(SMEM, pos), (VMEM, own), (VMEM, over_core(own))],
            [(VMEM, shape((size, width), F32))],
        )[0]

    grad, g_o, g_sum = call(
        first_grad_body,
        "first_grad",
        [(VMEM, cotangent.reshape(n, width))],
        [(VMEM, tok32), (VMEM, tok), (VMEM, shape((1, width), F32))],
    )
    collected = [None] * layers
    smalls = [None] * layers
    row1 = lambda cols: shape((1, cols), F32)
    for layer in reversed(range(layers)):
        s = saved[layer]
        wqkv, wout, w1, w2 = s["w"]
        g_t = over_x(g_o)

        def mlp_back(a, g, kind):
            return call(
                mlp_back_body,
                "mlp_back",
                [(VMEM, v) for v in (g, s["slope"][a], w2, w1)],
                [(VMEM, hid), (VMEM, kind), (VMEM, row1(ff))],
                (),
                gemm * 2 * ff,
            )

        dp_o, part, sum_o = mlp_back(0, g_o, tok32)
        dp_t, send, sum_t = mlp_back(1, g_t, tok)
        got = over_x(send)
        k1, s1, k2, s2 = call(
            mlp_grads_body,
            "mlp_grads",
            [(SMEM, pos)]
            + [
                (ANY, v)
                for v in (*s["act"], g_o, g_t, *s["mlp"], dp_o, dp_t)
            ],
            [(VMEM, shape((width, ff // 2)))] * 2 + [(VMEM, shape((ff, half)))] * 2,
            [
                pltpu.VMEM((2 * npad, width), BF16),
                pltpu.VMEM((2 * npad, ff), BF16),
                pltpu.VMEM((2 * npad, ff), BF16),
                pltpu.VMEM((2 * npad, width), BF16),
                sems((8,)),
            ],
            gemm * 4 * ff,
        )
        d_middle, ga_o, sums_b = call(
            norm_back_body,
            "norm_back",
            [(VMEM, v) for v in (part, got, s["middle"], gain(layer, 1), grad)],
            [(VMEM, tok32), (VMEM, tok), (VMEM, shape((3, width), F32))],
        )
        ga_t = over_x(ga_o)
        d_q, d_kv = call(
            attend_back_own_body,
            "attend_back_own",
            [(VMEM, v) for v in (ga_o, wout, *s["qkv"], s["probs"][0])],
            [(VMEM, ctx_s), (VMEM, shape((2 * npad, 2 * half), F32))],
            [kv_v, pltpu.VMEM((npad, half), BF16)],
            gemm * 4 * half,
        )
        mixed_o, mixed_t, send, sum_q = call(
            attend_back_other_body,
            "attend_back_other",
            [
                (VMEM, v)
                for v in (ga_t, wout, *s["qkv"], s["probs"][1], d_q, d_kv, wqkv)
            ],
            [(VMEM, qkv_s), (VMEM, qkv_s), (VMEM, tok), (VMEM, row1(3 * half))],
            [
                kv_v,
                pltpu.VMEM((npad, half), BF16),
                pltpu.VMEM((2 * npad, 2 * half), F32),
                pltpu.VMEM((npad, half), BF16),
            ],
            gemm * 7 * half,
        )
        got = over_x(send)
        part, kq, sq, ko, so = call(
            attend_grads_body,
            "attend_grads",
            [(SMEM, pos), (VMEM, mixed_o), (VMEM, wqkv)]
            + [(ANY, v) for v in (*s["ctx"], ga_o, ga_t, *s["ln"], mixed_o, mixed_t)],
            [(VMEM, tok32)]
            + [(VMEM, shape((width, 3 * half // 2)))] * 2
            + [(VMEM, shape((half, half)))] * 2,
            [
                pltpu.VMEM((2 * npad, half), BF16),
                pltpu.VMEM((2 * npad, width), BF16),
                pltpu.VMEM((2 * npad, width), BF16),
                pltpu.VMEM((2 * npad, 3 * half), BF16),
                sems((8,)),
            ],
            gemm * 11 * half,
        )
        grad, g_o, sums_a = call(
            norm_back_body,
            "norm_back",
            [(VMEM, v) for v in (part, got, s["stream"], gain(layer, 0), d_middle)],
            [(VMEM, tok32), (VMEM, tok), (VMEM, shape((3, width), F32))],
        )
        collected[layer] = (
            finish_columns(kq, sq, 3),
            finish_rows(ko, so, dg),
            finish_columns(k1, s1, 1),
            finish_rows(k2, s2, ffg),
        )
        plain = jnp.concatenate([sums_a[:1], sums_b[:1], sums_a[1:2], sums_b[2:3], sums_b[1:2], g_sum])
        plain = jnp.moveaxis(plain.reshape(6, group, dg), 1, 0)
        g_sum = sums_a[2:3]

        def place_heads(v, count=1):
            v = v.reshape(ys, 1, count, dg)
            out = jnp.where(
                (lax.broadcasted_iota(jnp.int32, (1, 2, 1, 1), 1) == x), v, 0.0
            )
            return out.reshape(group, count, dg)

        smalls[layer] = jnp.concatenate(
            [
                plain,
                place_heads(sum_q[:, :half]),
                place_heads(sum_q[:, 2 * half :]),
                place_heads(sum_o + sum_t, many),
            ],
            axis=1,
        )
    input_grad = g_o[:n].reshape(activations.shape)
    small_sum = jnp.concatenate(smalls, axis=1)
    for axis, mask_bit in [("replica", 1), ("group", 1)]:
        small_sum = small_sum + swap(small_sum, axis, mask_bit)
    k = 2
    while k < group:
        small_sum = small_sum + swap(small_sum, "group", k)
        k *= 2
    small_sum = lax.dynamic_index_in_dim(small_sum, me, 0, keepdims=False)
    k = 2
    while k < replica:
        small_sum = small_sum + swap(small_sum, "replica", k)
        k *= 2
    small_sum = small_sum.reshape(layers, 8 + many, dg)
    order = [2, 6, 7, 3, 4, 5]
    grad_biases = jnp.stack([small_sum[:, i] for i in order], axis=1)
    stacked = tuple(jnp.stack([collected[l][i] for l in range(layers)]) for i in range(4))
    return (
        outputs.reshape(activations.shape),
        input_grad,
        *stacked,
        small_sum[:, :2],
        grad_biases,
        small_sum[:, 8:].reshape(layers, many * dg),
    )


def solution(mesh):
    tokens = P("group", "replica", None, None)
    rows = P(None, "group", None)
    last = P(None, None, "group")
    return jax.shard_map(
        shards,
        mesh=mesh,
        in_specs=(
            tokens,
            P("group", "replica", None),
            rows,
            rows,
            rows,
            rows,
            last,
            last,
            P(None, "group"),
            tokens,
        ),
        out_specs=(tokens, tokens, rows, rows, rows, rows, last, last, P(None, "group")),
        check_vma=False,
    )
```

```python
import functools

import jax
import jax.numpy as jnp
from jax import lax
from jax.experimental import pallas as pl
from jax.experimental.pallas import tpu as pltpu
from jax.sharding import PartitionSpec as P

HEAD = 64
EPS = 1e-06
F32 = jnp.float32
BF16 = jnp.bfloat16
TILE = 256
ROWS = 16
MESH = pl.DeviceIdType.MESH
VMEM = pl.BlockSpec(memory_space=pltpu.VMEM)
SMEM = pl.BlockSpec(memory_space=pltpu.SMEM)
HBM = pl.BlockSpec(memory_space=pltpu.HBM)
SEMS = pltpu.SemaphoreType.DMA


def swap(value, axis, mask):
    pairs = [(source, source ^ mask) for source in range(lax.axis_size(axis))]
    return lax.ppermute(value, axis, pairs)


def dot(a, b):
    return lax.dot_general(a, b, (((1,), (0,)), ((), ())), preferred_element_type=F32)


def dot_nt(a, b):
    return lax.dot_general(a, b, (((1,), (1,)), ((), ())), preferred_element_type=F32)


def dot_tn(a, b):
    return lax.dot_general(a, b, (((0,), (0,)), ((), ())), preferred_element_type=F32)


def shape(dims, dtype=BF16):
    return jax.ShapeDtypeStruct(dims, dtype)


def padded(dims, dtype):
    size = dtype.itemsize if hasattr(dtype, "itemsize") else jnp.dtype(dtype).itemsize
    dims = list(dims)
    dims[-1] = -(-dims[-1] // 128) * 128
    if len(dims) > 1:
        dims[-2] = -(-dims[-2] // 16) * 16
    total = size
    for d in dims:
        total *= d
    return total


def call(body, name, ins, outs, scratch=(), flops=0, collective=None, extra=6, aliases=None, **kwargs):
    size = sum(a.size * a.dtype.itemsize for _, a in ins)
    size += sum(s.size * s.dtype.itemsize for _, s in outs)
    held = sum(padded(a.shape, a.dtype) for s, a in list(ins) + list(outs) if s is VMEM)
    held += sum(
        padded(s.shape, s.dtype) for s in scratch if getattr(s, "memory_space", None) == pltpu.VMEM
    )
    limit = min(held + extra * 2**20, 61 * 2**20)
    more = {}
    if collective is not None:
        more = dict(collective_id=collective, has_side_effects=True)
    return pl.pallas_call(
        functools.partial(body, **kwargs),
        name=name,
        in_specs=[s for s, _ in ins],
        out_specs=[s for s, _ in outs],
        out_shape=[s for _, s in outs],
        scratch_shapes=list(scratch),
        input_output_aliases=aliases or {},
        cost_estimate=pl.CostEstimate(flops=flops, bytes_accessed=size, transcendentals=0),
        compiler_params=pltpu.CompilerParams(vmem_limit_bytes=limit, **more),
    )(*[a for _, a in ins])


def loop(count, body):
    lax.fori_loop(0, count, lambda i, _: (body(i), None)[1], None)


def lanes(i, size=TILE):
    return pl.ds(pl.multiple_of(i * size, size), size)


def rows_at(start, size):
    return pl.ds(pl.multiple_of(start, size), size)


def chunk(i):
    return pl.ds(i * ROWS, ROWS)


def start_all(copies):
    for source, target, sem in copies:
        pltpu.make_async_copy(source, target, sem).start()


def wait_for(target, sem):
    pltpu.make_async_copy(target, target, sem).wait()


def pack_body(pos, *refs, layer, widths):
    ws, (theirs, ours, sem) = refs[:-3], refs[-3:]
    x, core = pos[0], pos[2]
    _, h, dg = ours.shape
    copies, at = [], 0
    rows = rows_at(core * h, h)
    for w, f in zip(ws, widths):
        for i in range(w.shape[2] // (2 * f)):
            for sub in range(f // dg):
                for k, (to, of) in enumerate(((theirs, 1 - x), (ours, x))):
                    col = pl.multiple_of((i * 2 + of) * f + sub * dg, dg)
                    copies.append((w.at[layer, rows, pl.ds(col, dg)], to.at[at], sem.at[k]))
                at += 1
    for w in ws[len(widths) :]:
        r = w.shape[1] // 2
        for part in range(r // h):
            for b in range(w.shape[2] // dg):
                source = w.at[layer, rows_at(core * r + part * h, h), pl.ds(b * dg, dg)]
                copies.append((source, ours.at[at], sem.at[1]))
                at += 1
    start_all(copies)
    wait_for(theirs, sem.at[0])
    wait_for(ours, sem.at[1])


def column_copies(pos, w, pieces, to, sem, layer, f):
    x, y, core = pos[0], pos[1], pos[2]
    dg = w.shape[1]
    h = dg // 2
    copies = []
    mine = rows_at((y * 2 + x) * dg, dg)
    for b in range(to.shape[1] // dg):
        i, sub = b * dg // f, b % (f // dg)
        cols = pl.ds(b * dg, dg)
        at = sem.at[b * dg // TILE]
        source = w.at[layer, :, pl.ds(pl.multiple_of((i * 2 + x) * f + sub * dg, dg), dg)]
        copies.append((source, to.at[mine, cols], at))
        for (yi, xi, ci), base, piece in pieces:
            row = ((y ^ yi) * 2 + (x ^ xi)) * dg + (core ^ ci) * h
            copies.append((piece.at[base + b], to.at[rows_at(row, h), cols], at))
    return copies


def row_copies(pos, w, pieces, to, sem, layer):
    y, core = pos[1], pos[2]
    r = w.shape[1]
    copies = [(w.at[layer], to.at[rows_at(y * r, r)], sem)]
    for (k, ci), base, piece in pieces:
        _, h, dg = piece.shape
        per = to.shape[1] // dg
        for part in range(r // 2 // h):
            row = (y ^ k) * r + (core ^ ci) * (r // 2) + part * h
            for b in range(per):
                target = to.at[rows_at(row, h), pl.ds(b * dg, dg)]
                copies.append((piece.at[base + part * per + b], target, sem))
    return copies


def layer_norm_rows(v, gain, shift):
    mean = jnp.mean(v, axis=-1, keepdims=True)
    centred = v - mean
    var = jnp.mean(centred * centred, axis=-1, keepdims=True)
    return (centred * lax.rsqrt(var + EPS) * gain + shift).astype(BF16)


def first_norm_body(act_o, act_t, gain, shift, stream, ln_o, ln_t):
    for i in range(act_o.shape[0] // ROWS):
        v = act_o[chunk(i), :].astype(F32)
        stream[chunk(i), :] = v
        ln_o[chunk(i), :] = layer_norm_rows(v, gain[...], shift[...])
        ln_t[chunk(i), :] = layer_norm_rows(act_t[chunk(i), :].astype(F32), gain[...], shift[...])


def norm_body(base, part, got, bias, gain, shift, stream, ln):
    for i in range(base.shape[0] // ROWS):
        v = base[chunk(i), :] + (part[chunk(i), :] + got[chunk(i), :].astype(F32)) + bias[...]
        stream[chunk(i), :] = v
        ln[chunk(i), :] = layer_norm_rows(v, gain[...], shift[...])


def last_body(base, part, got, bias, out):
    n = out.shape[0]
    for i in range(-(-n // ROWS)):
        v = base[chunk(i), :] + (part[chunk(i), :] + got[chunk(i), :].astype(F32)) + bias[...]
        size = min(ROWS, n - i * ROWS)
        out[pl.ds(i * ROWS, size), :] = v.astype(BF16)[:size]


def pad_rows_body(v, mask, out):
    n = v.shape[0]
    out[...] = jnp.zeros_like(out)
    out[0:n, :] = v[...]
    out[out.shape[0] - 1 : out.shape[0], :] = mask[...]


def pad_grad_body(v, out, sums):
    n = v.shape[0]
    out[...] = jnp.zeros_like(out)
    out[0:n, :] = v[...]
    sums[...] = jnp.sum(v[...].astype(F32), axis=0, keepdims=True)


def norm_back_body(part, got, base, gain, before, after, g, sums):
    n, width = g.shape
    totals = [jnp.zeros((8, width), F32)] * 3
    for i in range(n // ROWS):
        d = part[chunk(i), :] + got[chunk(i), :].astype(F32)
        v = base[chunk(i), :]
        mean = jnp.mean(v, axis=-1, keepdims=True)
        centred = v - mean
        var = jnp.mean(centred * centred, axis=-1, keepdims=True)
        inv = lax.rsqrt(var + EPS)
        xhat = centred * inv
        e = d * gain[...]
        m1 = jnp.mean(e, axis=-1, keepdims=True)
        m2 = jnp.mean(e * xhat, axis=-1, keepdims=True)
        r = before[chunk(i), :].astype(F32) + (e - m1 - xhat * m2) * inv
        low = r.astype(BF16)
        if after is not None:
            after[chunk(i), :] = r
        g[chunk(i), :] = low
        terms = (d * xhat, d, low.astype(F32))
        totals = [t + (v[:8] + v[8:]) for t, v in zip(totals, terms)]
    for k, t in enumerate(totals):
        sums[k : k + 1, :] = jnp.sum(t, axis=0, keepdims=True)


def project(ln, w, bias, out, width, sem=None):
    def step(i):
        if sem is not None:
            wait_for(w.at[:, lanes(i)], sem.at[i])
        v = dot(ln[...], w[:, lanes(i)]) + bias[:, lanes(i)]
        factor = jnp.where(i * TILE < width, HEAD ** (-0.5), 1.0)
        out[:, lanes(i)] = (v * factor).astype(BF16)

    loop(out.shape[1] // TILE, step)


def qkv_body(pos, ln, bias, w_all, *refs, layer, keys, f):
    pieces, (out, w, sem) = refs[:-3], refs[-3:]
    pieces = [(k, b, p) for (k, b), p in zip(keys, pieces)]
    start_all(column_copies(pos, w_all, pieces, w, sem, layer, f))
    project(ln, w, bias, out, out.shape[1] // 3, sem)


def attend(q, kv, mask, probs, ctx, width):
    first = lax.broadcasted_iota(jnp.int32, (1, 2 * HEAD), 1) < HEAD
    for hp in range(width // (2 * HEAD)):
        cols = slice(hp * 2 * HEAD, (hp + 1) * 2 * HEAD)
        q2 = q[:, cols]
        k2 = kv[:, cols]
        v2 = kv[:, slice(width + cols.start, width + cols.stop)]
        outs = []
        for e in range(2):
            keep = first if e == 0 else jnp.logical_not(first)
            s = dot_nt(jnp.where(keep, q2, jnp.zeros_like(q2)), k2) + mask[...]
            top = jnp.max(s, axis=-1, keepdims=True)
            ex = jnp.exp(s - top)
            p = (ex * (1.0 / jnp.sum(ex, axis=-1, keepdims=True))).astype(BF16)
            probs[hp * 2 + e] = p
            outs.append(dot(p, v2))
        ctx[:, cols] = jnp.where(first, outs[0], outs[1]).astype(BF16)


def join(own, other, kv, width):
    n = own.shape[0]
    kv[0:n, :] = own[:, width:]
    kv[n:, :] = other[:, width:]


def matmul(a, w, out):
    def step(i):
        out[:, lanes(i)] = dot(a[...], w[:, lanes(i)]).astype(out.dtype)

    loop(out.shape[1] // TILE, step)


def matmul_nt(a, w, out):
    def step(i):
        out[:, lanes(i)] = dot_nt(a[...], w[lanes(i), :]).astype(out.dtype)

    loop(out.shape[1] // TILE, step)


def attend_other_body(pos, ln, w, bias, own, mask, wout_all, *refs, layer, keys):
    pieces, (qkv, probs, ctx, partial, wout, kv, sem) = refs[:-7], refs[-7:]
    width = ctx.shape[1]
    pieces = [(k, b, p) for (k, b), p in zip(keys, pieces)]
    start_all(row_copies(pos, wout_all, pieces, wout, sem.at[0], layer))
    project(ln, w, bias, qkv, width)
    join(own, qkv, kv, width)
    attend(qkv.at[:, 0:width], kv, mask, probs, ctx, width)
    wait_for(wout, sem.at[0])
    matmul(ctx, wout, partial)


def attend_own_body(own, other, mask, wout, probs, ctx, partial, kv):
    width = ctx.shape[1]
    join(own, other, kv, width)
    attend(own.at[:, 0:width], kv, mask, probs, ctx, width)
    matmul(ctx, wout, partial)


def hidden(mlp, w1, bias, act, slope, sem):
    def step(i):
        wait_for(w1.at[:, lanes(i)], sem.at[i])
        v = dot(mlp[...], w1[:, lanes(i)]) + bias[:, lanes(i)]
        cdf = 0.5 * (1.0 + lax.erf(v * (0.5**0.5)))
        pdf = jnp.exp(-0.5 * v * v) * 0.3989422804014327
        act[:, lanes(i)] = (v * cdf).astype(BF16)
        slope[:, lanes(i)] = (cdf + v * pdf).astype(BF16)

    loop(act.shape[1] // TILE, step)


def mlp_own_body(pos, mlp, bias, w1_all, w2_all, *refs, layer, keys1, keys2, f):
    pieces, (act, slope, partial, w1, w2, sem) = refs[:-6], refs[-6:]
    tiles = act.shape[1] // TILE
    one = [(k, b, p) for (k, b), p in zip(keys1, pieces)]
    two = [(k, b, p) for (k, b), p in zip(keys2, pieces[len(keys1) :])]
    start_all(column_copies(pos, w1_all, one, w1, sem, layer, f))
    start_all(row_copies(pos, w2_all, two, w2, sem.at[tiles], layer))
    hidden(mlp, w1, bias, act, slope, sem)
    wait_for(w2, sem.at[tiles])
    matmul(act, w2, partial)


def start_tiles(source, target, sem, by_rows=False):
    def step(i):
        at = (lanes(i), slice(None)) if by_rows else (slice(None), lanes(i))
        pltpu.make_async_copy(source.at[at], target.at[at], sem.at[i]).start()

    loop(target.shape[0 if by_rows else 1] // TILE, step)


def mlp_other_body(mlp, bias, w1_in, w2_in, act, slope, partial, w1, w2, sem):
    tiles = act.shape[1] // TILE
    start_tiles(w1_in, w1, sem)
    pltpu.make_async_copy(w2_in, w2, sem.at[tiles]).start()
    hidden(mlp, w1, bias, act, slope, sem)
    wait_for(w2, sem.at[tiles])
    matmul(act, w2, partial)


def mlp_back_body(g, slope, w2_in, w1_in, d_pre, d_mlp, sums, w2, w1, sem):
    tiles = d_pre.shape[1] // TILE
    start_tiles(w2_in, w2, sem, True)
    pltpu.make_async_copy(w1_in, w1, sem.at[tiles]).start()

    def step(i):
        wait_for(w2.at[lanes(i), :], sem.at[i])
        v = dot_nt(g[...], w2[lanes(i), :]) * slope[:, lanes(i)].astype(F32)
        v = v.astype(BF16)
        d_pre[:, lanes(i)] = v
        sums[:, lanes(i)] = jnp.sum(v.astype(F32), axis=0, keepdims=True)

    loop(tiles, step)
    wait_for(w1, sem.at[tiles])
    matmul_nt(d_pre, w1, d_mlp)


def load_pairs(pairs, sem):
    for i, ((own, other), buffer) in enumerate(pairs):
        n = own.shape[0]
        start_all([(own, buffer.at[0:n], sem.at[i]), (other, buffer.at[n:], sem.at[i])])
    return lambda i: wait_for(pairs[i][1], sem.at[i])


def meet(*partners):
    barrier = pltpu.get_barrier_semaphore()
    for p in partners:
        pl.semaphore_signal(barrier, 1, device_id=p, device_id_type=MESH)
    pl.semaphore_wait(barrier, len(partners))


def place_of():
    me, rep = lax.axis_index("group"), lax.axis_index("replica")
    return lax.rem(me, 2), me // 2, lax.rem(rep, 2), rep // 2


def grads(parts, outs, sent, got, send_sem, recv_sem):
    x, y, core, z = place_of()
    other = {"replica": 2 * z + 1 - core}
    meet(other)
    ys = len(outs)

    def run(half, finish):
        count = 0
        for tiles, make in parts:
            for t in range(tiles):
                finish(count, make(t, half))
                count += 1

    def copy(i, at):
        k, rows, cols = at
        return pltpu.make_async_remote_copy(
            sent.at[k, rows, cols],
            got.at[k, rows, cols],
            send_sem.at[i],
            recv_sem.at[i],
            device_id=other,
            device_id_type=MESH,
        )

    index = [0]
    copies = []

    def send(_, blocks):
        for (k, rows, cols), value in blocks:
            sent[k, rows, cols] = value.astype(BF16)
            c = copy(index[0], (k, rows, cols))
            c.start()
            copies.append(c)
            index[0] += 1

    run(1 - core, send)
    index[0] = 0

    def keep(_, blocks):
        for (k, rows, cols), value in blocks:
            copies[index[0]].wait_recv()
            outs[k][rows, cols] = (value + got[k, rows, cols].astype(F32)).astype(BF16)
            index[0] += 1

    run(core, keep)
    for c in copies:
        c.wait_send()
    del ys


def column_part(lhs, rhs, parts, ys, at, base_rows):
    x, y, core, z = place_of()
    rows = lhs.shape[1] // ys
    cols = rhs.shape[1] // (2 * parts)
    per = cols // TILE

    def make(t, half):
        p, q = t // per, t % per
        start = pl.multiple_of(p * 2 * cols + half * cols + q * TILE, TILE)
        r = rhs[:, pl.ds(start, TILE)]
        return [
            (
                (k, slice(base_rows, base_rows + rows), slice(at + t * TILE, at + (t + 1) * TILE)),
                dot_tn(lhs[:, rows_at((y ^ k) * rows, rows)], r),
            )
            for k in range(ys)
        ]

    return parts * per, make


def row_part(lhs, rhs, ys, spot):
    x, y, core, z = place_of()
    rows = lhs.shape[1] // ys
    half_cols = rhs.shape[1] // 2

    def make(t, half):
        r = rhs[:, pl.ds(pl.multiple_of(half * half_cols + t * TILE, TILE), TILE)]
        out = []
        for k in range(ys):
            count = spot(t, None)
            size = rows // count
            for i in range(count):
                start = (y ^ k) * rows + i * size
                to_rows, to_cols = spot(t, i)
                out.append(((k, to_rows, to_cols), dot_tn(lhs[:, rows_at(start, size)], r)))
        return out

    return half_cols // TILE, make


def mlp_grads_body(*refs, ys):
    ins, outs, rest = refs[:8], refs[8 : 8 + ys], refs[8 + ys :]
    mlp, d_pre, act, g, sent, got, sem, send_sem, recv_sem = rest
    pairs = [(ins[2 * i : 2 * i + 2], b) for i, b in enumerate((act, g, mlp, d_pre))]
    wait = load_pairs(pairs, sem)
    for i in range(4):
        wait(i)
    rows = mlp.shape[1] // ys
    half = g.shape[1] // 2

    def spot(t, i):
        if i is None:
            return 2
        return slice(rows, 2 * rows), slice(i * half + t * TILE, i * half + (t + 1) * TILE)

    parts = [column_part(mlp, d_pre, 1, ys, 0, 0), row_part(act, g, ys, spot)]
    grads(parts, outs, sent, got, send_sem, recv_sem)


def attend_grads_body(mixed, w, *refs, ys):
    ins, d_ln, outs, rest = refs[:8], refs[8], refs[9 : 9 + ys], refs[9 + ys :]
    ctx, ga, ln, d_mixed, sent, got, sem, send_sem, recv_sem = rest
    pairs = [(ins[2 * i : 2 * i + 2], b) for i, b in enumerate((ctx, ga, ln, d_mixed))]
    wait = load_pairs(pairs, sem)
    matmul_nt(mixed, w, d_ln)
    for i in range(4):
        wait(i)
    rows = ctx.shape[1] // ys
    at = d_mixed.shape[1] // 2

    def spot(t, i):
        if i is None:
            return 1
        return slice(t * rows, (t + 1) * rows), slice(at, at + TILE)

    parts = [column_part(ln, d_mixed, 3, ys, 0, 0), row_part(ctx, ga, ys, spot)]
    grads(parts, outs, sent, got, send_sem, recv_sem)


def attend_back(ga, wout, q, kv, probs, d_ctx, d_q, d_kv, width):
    matmul_nt(ga, wout, d_ctx)
    first = lax.broadcasted_iota(jnp.int32, (1, 2 * HEAD), 1) < HEAD
    for hp in range(width // (2 * HEAD)):
        cols = slice(hp * 2 * HEAD, (hp + 1) * 2 * HEAD)
        vcols = slice(width + cols.start, width + cols.stop)
        q2, k2, v2, c2 = q[:, cols], kv[:, cols], kv[:, vcols], d_ctx[:, cols]
        dq, dk, dv = [], [], []
        for e in range(2):
            keep = first if e == 0 else jnp.logical_not(first)
            p = probs[hp * 2 + e]
            d = dot_nt(jnp.where(keep, c2, jnp.zeros_like(c2)), v2)
            pf = p.astype(F32)
            delta = jnp.sum(pf * d, axis=-1, keepdims=True)
            ds = (pf * (d - delta)).astype(BF16)
            dq.append(dot(ds, k2))
            dk.append(dot_tn(ds, q2))
            dv.append(dot_tn(p, c2))
        d_q[:, cols] = (
            jnp.where(first, dq[0], dq[1]).astype(BF16).astype(F32) * HEAD ** (-0.5)
        ).astype(BF16)
        d_kv[:, cols] += jnp.where(first, dk[0], dk[1])
        d_kv[:, vcols] += jnp.where(first, dv[0], dv[1])


def attend_back_own_body(ga, wout, own, other, probs, d_q, d_kv, kv, d_ctx):
    width = d_q.shape[1]
    join(own, other, kv, width)
    d_kv[...] = jnp.zeros_like(d_kv)
    attend_back(ga, wout, own.at[:, 0:width], kv, probs, d_ctx, d_q, d_kv, width)


def attend_back_other_body(
    ga, wout, own, other, probs, d_q, d_kv_in, w, mixed_o, mixed_t, d_ln, sums, kv, d_ctx, d_kv, d_qt
):
    width = d_q.shape[1]
    n = own.shape[0]
    join(own, other, kv, width)
    d_kv[...] = d_kv_in[...]
    attend_back(ga, wout, other.at[:, 0:width], kv, probs, d_ctx, d_qt, d_kv, width)
    mixed_o[:, 0:width] = d_q[...]
    mixed_t[:, 0:width] = d_qt[...]
    mixed_o[:, width:] = d_kv[0:n, :].astype(BF16)
    mixed_t[:, width:] = d_kv[n:, :].astype(BF16)
    matmul_nt(mixed_t, w, d_ln)
    for at in range(0, 3 * width, width):
        cols = slice(at, at + width)
        sums[:, cols] = jnp.sum(mixed_o[:, cols].astype(F32), axis=0, keepdims=True) + jnp.sum(
            mixed_t[:, cols].astype(F32), axis=0, keepdims=True
        )


def tail_body(*refs, ys, zs, done_layers, dg, pieces, lag):
    it = iter(refs)
    mlp_keep = next(it)
    mlp_got = [next(it) for _ in range(ys - 1)]
    att_keep = next(it)
    att_send = [next(it) for _ in range(ys - 1)]
    small_in = next(it)
    done = [next(it) for _ in range(done_layers)]
    total = next(it)
    xr = [next(it) for _ in range(done_layers + 1)]
    cr = [next(it) for _ in range(done_layers + 1)]
    small_out = next(it)
    part, up, hub = next(it), next(it), next(it)
    att_got = [next(it) for _ in range(ys - 1)]
    small, small_got = next(it), next(it)
    y_send, y_recv, s_send, s_recv = next(it), next(it), next(it), next(it)
    v_send, u_recv, h_recv, t_send, t_recv = (next(it) for _ in range(5))
    f_send, f_recv = next(it), next(it)

    x, y, core, z = place_of()
    size, width = total.shape
    qc = 3 * width // 4
    left = z < zs // 2
    q = jnp.where(left, z, zs - 1 - z)
    is_hub = q == zs // 2 - 1
    has_outer = q > 0
    inner = {"replica": 2 * jnp.where(left, z + 1, z - 1) + core}
    outer = {"replica": 2 * jnp.where(left, jnp.maximum(z - 1, 0), jnp.minimum(z + 1, zs - 1)) + core}
    mate = {"replica": 2 * z + 1 - core}
    across = {"group": 2 * y + 1 - x}
    beyond = [{"group": 2 * (y ^ k) + x} for k in range(1, ys)]

    barrier = pltpu.get_barrier_semaphore()
    for p in [inner, mate, across, *beyond]:
        pl.semaphore_signal(barrier, 1, device_id=p, device_id_type=MESH)

    @pl.when(has_outer)
    def _():
        pl.semaphore_signal(barrier, 1, device_id=outer, device_id_type=MESH)

    pl.semaphore_wait(barrier, 3 + len(beyond) + jnp.where(has_outer, 1, 0))

    def remote(source, target, send, recv, device):
        return pltpu.make_async_remote_copy(
            source, target, send, recv, device_id=device, device_id_type=MESH
        )

    y_copies = [
        remote(att_send[k], att_got[k], y_send.at[k], y_recv.at[k], beyond[k]) for k in range(ys - 1)
    ]

    fc1 = rows_at(x * dg, dg)
    fc1_x = rows_at((1 - x) * dg, dg)
    att = rows_at(4 * dg + x * dg, dg)
    att_x = rows_at(4 * dg + (1 - x) * dg, dg)

    def x_copies(layer, v):
        s = 6 * layer
        return (
            remote(v.at[fc1_x], xr[layer].at[0:dg], f_send.at[s], f_recv.at[s], across),
            remote(
                v.at[att_x, 0:qc],
                xr[layer].at[dg : 2 * dg, 0:qc],
                f_send.at[s + 1],
                f_recv.at[s + 1],
                across,
            ),
        )

    def core_copies(layer, v):
        s = 6 * layer
        return (
            remote(v.at[0 : 4 * dg], cr[layer].at[0 : 4 * dg], f_send.at[s + 2], f_recv.at[s + 2], mate),
            remote(
                v.at[4 * dg : 6 * dg],
                cr[layer].at[4 * dg : 6 * dg],
                f_send.at[s + 3],
                f_recv.at[s + 3],
                mate,
            ),
        )

    def forward_copies(layer):
        s = 6 * layer
        return (
            remote(
                xr[layer].at[0:dg],
                cr[layer].at[6 * dg : 7 * dg],
                f_send.at[s + 4],
                f_recv.at[s + 4],
                mate,
            ),
            remote(
                xr[layer].at[dg : 2 * dg],
                cr[layer].at[7 * dg : 8 * dg],
                f_send.at[s + 5],
                f_recv.at[s + 5],
                mate,
            ),
        )

    at = 2 + ys.bit_length() - 1
    n_small = at
    step = size // pieces
    mlp_pieces = pieces * 4 // 6

    def rows_of(i):
        return slice(i * step, (i + 1) * step)

    def own_part(i):
        r = rows_of(i)
        if i < mlp_pieces:
            v = mlp_keep[r, :].astype(F32)
            for g in mlp_got:
                v = v + g[r, :].astype(F32)
        else:
            a = slice(i * step - 4 * dg, (i + 1) * step - 4 * dg)
            v = att_keep[a, :].astype(F32)
            for g in att_got:
                v = v + g[a, :].astype(F32)
        return v

    def send_in(i):
        r = rows_of(i)

        @pl.when(is_hub)
        def _():
            remote(part.at[r], hub.at[r], v_send.at[i], h_recv.at[i], inner).start()

        @pl.when(jnp.logical_not(is_hub))
        def _():
            remote(part.at[r], up.at[r], v_send.at[i], u_recv.at[i], inner).start()

    def inward_end(i):
        part[rows_of(i), :] = own_part(i).astype(BF16)
        send_in(i)

    def inward(i):
        r = rows_of(i)
        v = own_part(i)
        remote(part.at[r], up.at[r], v_send.at[i], u_recv.at[i], outer).wait_recv()
        part[r, :] = (v + up[r, :].astype(F32)).astype(BF16)
        send_in(i)

    def outward(i):
        r = rows_of(i)

        @pl.when(is_hub)
        def _():
            remote(part.at[r], hub.at[r], v_send.at[i], h_recv.at[i], inner).wait_recv()
            total[r, :] = (part[r, :].astype(F32) + hub[r, :].astype(F32)).astype(BF16)

        @pl.when(jnp.logical_not(is_hub))
        def _():
            remote(total.at[r], total.at[r], t_send.at[i], t_recv.at[i], inner).wait_recv()

        @pl.when(has_outer)
        def _():
            remote(total.at[r], total.at[r], t_send.at[i], t_recv.at[i], outer).start()

    small_up, small_hub, small_total = n_small, n_small + 1, n_small + 1

    def small_inward():
        @pl.when(has_outer)
        def _():
            remote(
                small.at[n_small], small_got.at[small_up], s_send.at[at], s_recv.at[at], outer
            ).wait_recv()
            small[n_small] = small[n_small] + small_got[small_up]

        @pl.when(is_hub)
        def _():
            remote(
                small.at[n_small], small_got.at[small_hub], s_send.at[at], s_recv.at[at + 1], inner
            ).start()

        @pl.when(jnp.logical_not(is_hub))
        def _():
            remote(
                small.at[n_small], small_got.at[small_up], s_send.at[at], s_recv.at[at], inner
            ).start()

    def small_outward():
        @pl.when(is_hub)
        def _():
            remote(
                small.at[n_small], small_got.at[small_hub], s_send.at[at], s_recv.at[at + 1], inner
            ).wait_recv()
            small[small_total] = small[n_small] + small_got[small_hub]

        @pl.when(jnp.logical_not(is_hub))
        def _():
            remote(
                small.at[small_total], small.at[small_total], s_send.at[at + 1], s_recv.at[at + 2], inner
            ).wait_recv()

        @pl.when(has_outer)
        def _():
            remote(
                small.at[small_total], small.at[small_total], s_send.at[at + 1], s_recv.at[at + 2], outer
            ).start()

    forwarded = []

    def finish_up():
        for layer, v, xs, cs in finished:
            fwd = forward_copies(layer)
            for c in xs:
                c.wait_recv()
            for c in fwd:
                c.start()
            forwarded.extend(cs + fwd)

    at_end = jnp.logical_not(has_outer)

    @pl.when(at_end)
    def _():
        for i in range(mlp_pieces):
            inward_end(i)

    small[0] = small_in[...]
    s_copies = []
    for i, device in enumerate([mate, across]):
        c = remote(small.at[i], small_got.at[i], s_send.at[i], s_recv.at[i], device)
        c.start()
        c.wait_recv()
        s_copies.append(c)
        small[i + 1] = small[i] + small_got[i]
    i = 2
    k = 1
    while k < ys:
        c = remote(small.at[i], small_got.at[i], s_send.at[i], s_recv.at[i], beyond[k - 1])
        c.start()
        c.wait_recv()
        s_copies.append(c)
        small[i + 1] = small[i] + small_got[i]
        i += 1
        k *= 2

    for c in y_copies:
        c.start()
    finished = []
    for i in range(done_layers):
        layer = i + 1
        xs, cs = x_copies(layer, done[i]), core_copies(layer, done[i])
        for c in xs + cs:
            c.start()
        finished.append((layer, done[i], xs, cs))

    @pl.when(at_end)
    def _():
        for c in y_copies:
            c.wait_recv()
        for i in range(mlp_pieces, pieces):
            inward_end(i)
        small_inward()

    l0 = {}
    for i in range(pieces + lag):

        @pl.when(has_outer)
        def _():
            if i == mlp_pieces:
                for c in y_copies:
                    c.wait_recv()
            if i < pieces:
                inward(i)
            if i == pieces - 1:
                small_inward()

        if i >= lag:
            outward(i - lag)
            if i - lag == mlp_pieces - 1:
                l0["x1"], l0["x2"] = x_copies(0, total)
                l0["c1"], l0["c2"] = core_copies(0, total)
                l0["x1"].start()
                l0["c1"].start()
        if i == mlp_pieces - 1:
            finish_up()
    l0["x2"].start()
    l0["c2"].start()
    small_outward()
    l0["f1"], l0["f2"] = forward_copies(0)
    l0["x1"].wait_recv()
    l0["f1"].start()
    l0["x2"].wait_recv()
    l0["f2"].start()
    for c in [l0["c1"], l0["c2"], l0["f1"], l0["f2"]] + forwarded:
        c.wait_recv()
    small_out[...] = small[small_total, 2 * y + x]

    for c in y_copies + s_copies + list(l0.values()):
        c.wait_send()
    for layer, v, xs, cs in finished:
        for c in xs:
            c.wait_send()
    for c in forwarded:
        c.wait_send()
    for i in range(pieces):
        r = rows_of(i)
        remote(part.at[r], up.at[r], v_send.at[i], u_recv.at[i], inner).wait_send()

        @pl.when(has_outer)
        def _():
            remote(total.at[r], total.at[r], t_send.at[i], t_recv.at[i], outer).wait_send()

    remote(small.at[n_small], small_got.at[small_up], s_send.at[at], s_recv.at[at], inner).wait_send()

    @pl.when(has_outer)
    def _():
        remote(
            small.at[small_total], small.at[small_total], s_send.at[at + 1], s_recv.at[at + 2], outer
        ).wait_send()


def tail(mlp_keep, mlp_got, att, small, done, *, ys, zs, dg, pieces=24, lag=3):
    width = mlp_keep.shape[1]
    layers = len(done) + 1
    levels = 3 + max(ys.bit_length() - 1, 1) + 2
    whole = (6 * dg, width)
    total, *rest = call(
        tail_body,
        "tail",
        [(VMEM, v) for v in (mlp_keep, *mlp_got, *att, small, *done)],
        [(VMEM, shape(whole))]
        + [(VMEM, shape((2 * dg, width)))] * layers
        + [(VMEM, shape((8 * dg, width)))] * layers
        + [(VMEM, shape(small.shape[1:], F32))],
        [pltpu.VMEM(whole, BF16)] * 3
        + [pltpu.VMEM((2 * dg, width), BF16)] * (ys - 1)
        + [pltpu.VMEM((levels, *small.shape), F32)] * 2
        + [SEMS((ys,)), SEMS((ys,)), SEMS((levels + 1,)), SEMS((levels + 2,))]
        + [SEMS((pieces,))] * 5
        + [SEMS((6 * layers,))] * 2,
        collective=2,
        ys=ys,
        zs=zs,
        done_layers=layers - 1,
        dg=dg,
        pieces=pieces,
        lag=lag,
    )
    mine = [total] + list(done)
    return list(zip(mine, rest[:layers], rest[layers : 2 * layers])), rest[2 * layers]


def place_body(pos, *refs, ys):
    x, core = pos[0], pos[2]
    inputs, (fc1, fc2, qkv, out) = refs[:-4], refs[-4:]
    per = ys // 2
    for layer in range(len(inputs) // 3):
        v, xr, cr = inputs[3 * layer : 3 * layer + 3]
        width = v.shape[1]
        dg = v.shape[0] // 6
        half, quarter = width // 2, width // 4
        qc = 3 * quarter
        my_fc1, my_att = rows_at(x * dg, dg), rows_at(4 * dg + x * dg, dg)
        for c, w, x1, x2 in (
            (core, v, (xr, 0), (xr, dg)),
            (1 - core, cr, (cr, 6 * dg), (cr, 7 * dg)),
        ):
            f = 4 * dg
            for b, src in ((0, w[my_fc1, :]), (1, x1[0][x1[1] : x1[1] + dg, :])):
                for j in range(per):
                    at = pl.multiple_of(((c * per + j) * 2 + (x ^ b)) * f, f)
                    fc1[layer, :, pl.ds(at, f)] = src[:, j * f : (j + 1) * f].astype(F32)
            for a in range(2):
                fc2[layer, a * 2 * dg : (a + 1) * 2 * dg, lanes(c, half)] = w[
                    2 * dg : 4 * dg, a * half : (a + 1) * half
                ].astype(F32)
                out[layer, :, lanes(2 * c + a, quarter)] = w[
                    4 * dg + a * dg : 4 * dg + (a + 1) * dg, qc:
                ].astype(F32)
            for b, src in ((0, w[my_att, 0:qc]), (1, x2[0][x2[1] : x2[1] + dg, 0:qc])):
                for p in range(3):
                    for j in range(per):
                        at = pl.multiple_of(((p * ys + c * per + j) * 2 + (x ^ b)) * dg, dg)
                        i = p * per + j
                        qkv[layer, :, pl.ds(at, dg)] = src[:, i * dg : (i + 1) * dg].astype(F32)


def shards(
    activations,
    key_mask,
    qkv_weight,
    out_weight,
    fc1_weight,
    fc2_weight,
    ln_gains,
    biases,
    fc1_bias,
    cotangent,
):
    layers = qkv_weight.shape[0]
    n = activations.shape[2]
    npad = -(-(n + 1) // ROWS) * ROWS
    width = activations.shape[3]
    half = width // 2
    group, replica = lax.axis_size("group"), lax.axis_size("replica")
    ys, zs = group // 2, replica // 2
    dg = width // group
    h = dg // 2
    ffg = fc2_weight.shape[1]
    ff = ffg * ys
    many = ffg // dg
    heads = half // HEAD
    me, rep = lax.axis_index("group"), lax.axis_index("replica")
    x, y = me % 2, me // 2
    core = rep % 2
    pos = jnp.stack([x, y, core]).astype(jnp.int32)

    def over_x(v):
        return swap(v, "group", 1)

    def over_y(v, k):
        return swap(v, "group", 2 * k)

    def over_core(v):
        return swap(v, "replica", 1)

    def pack(layer, columns, rows):
        ws = [w for w, _ in columns] + rows
        nx = sum(w.shape[2] // 2 // dg for w, _ in columns)
        ny = nx + sum(w.shape[1] // dg * group for w in rows)
        theirs, ours = call(
            pack_body,
            "pack",
            [(SMEM, pos)] + [(HBM, w) for w in ws],
            [(VMEM, shape((nx, h, dg))), (VMEM, shape((ny, h, dg)))],
            [SEMS((2,))],
            layer=layer,
            widths=[f for _, f in columns],
        )

        def exchange(after=None):
            first, second = theirs, ours
            if after is not None:
                first, second, _ = lax.optimization_barrier((theirs, ours, after))
            arrays = {(0, 1): over_x(first)}
            for k in range(1, ys):
                arrays[k, 0] = over_y(second, k)
            for k in range(1, ys):
                arrays[k, 1] = over_y(arrays[0, 1], k)
            for key, v in list(arrays.items()):
                arrays[key + (0,)] = v
                arrays[key + (1,)] = over_core(v)
                del arrays[key]
            out, base = [], 0
            for w, _ in columns:
                out.append(([(key, base) for key in arrays], list(arrays.values())))
                base += w.shape[2] // 2 // dg
            for w in rows:
                keys = [(k, c) for k in range(1, ys) for c in range(2)]
                out.append(([(key, base) for key in keys], [arrays[k, 0, c] for k, c in keys]))
                base += w.shape[1] // dg * group
            return out

        return exchange

    small = jnp.concatenate(
        [
            ln_gains.reshape(layers * 2, dg),
            biases.reshape(layers * 6, dg),
            fc1_bias.reshape(layers * many, dg),
        ],
        axis=0,
    )
    small_x = over_x(small)
    small = jnp.where(x == 0, jnp.stack([small, small_x]), jnp.stack([small_x, small]))
    small = small[None]
    k = 1
    while k < ys:
        other = over_y(small, k)
        small = jnp.where(
            (y & k) == 0,
            jnp.concatenate([small, other], axis=0),
            jnp.concatenate([other, small], axis=0),
        )
        k *= 2

    mask_o = jnp.pad(key_mask.reshape(1, n), ((0, 0), (0, width - n))).astype(BF16)
    act_o = call(
        pad_rows_body,
        "pad",
        [(VMEM, activations.reshape(n, width)), (VMEM, mask_o)],
        [(VMEM, shape((npad, width)))],
    )[0]
    fetched = {}
    fetched[0, "a"] = pack(0, [(qkv_weight, dg)], [out_weight])()
    act_t = over_x(act_o)
    packs = {(0, "m"): pack(0, [(fc1_weight, ffg)], [fc2_weight])}
    for layer in range(1, layers):
        packs[layer, "a"] = pack(layer, [(qkv_weight, dg)], [out_weight])
        packs[layer, "m"] = pack(layer, [(fc1_weight, ffg)], [fc2_weight])
    fetched[0, "m"] = packs[0, "m"](act_t[:ROWS])
    mask_t = act_t[npad - 1 :, :npad]
    mask = jnp.concatenate([mask_o[:, :npad], mask_t], axis=1)
    mask = jnp.where(mask > 0, 0.0, -1e30).astype(F32)

    blocks = small.reshape(group, -1, dg)
    rows_all = jnp.moveaxis(blocks[:, : layers * 8], 0, 1).reshape(layers * 8, width).astype(F32)
    mine = lax.dynamic_index_in_dim(small, x, 1, keepdims=False).astype(F32)

    def gain(layer, i):
        return rows_all[layer * 2 + i][None]

    def shift(layer, i):
        return rows_all[layers * 2 + layer * 6 + i][None]

    def head_shift(layer):
        at = layers * 2 + layer * 6
        q, v = mine[:, at + 1].reshape(1, half), mine[:, at + 2].reshape(1, half)
        return jnp.concatenate([q, jnp.zeros_like(q), v], axis=1)

    def fc1_shift(layer):
        at = layers * 8 + layer * many
        return mine[:, at : at + many].reshape(1, ff)

    tok = shape((npad, width))
    tok32 = shape((npad, width), F32)
    qkv_s = shape((npad, 3 * half))
    probs_s = shape((heads, npad, 2 * npad))
    ctx_s = shape((npad, half))
    hid = shape((npad, ff))
    kv_v = pltpu.VMEM((2 * npad, 2 * half), BF16)
    gemm = 2 * npad * width
    tiles = ff // TILE

    saved = []
    stream, ln_o, ln_t = call(
        first_norm_body,
        "norm_first",
        [(VMEM, act_o), (VMEM, act_t), (VMEM, gain(0, 0)), (VMEM, shift(0, 0))],
        [(VMEM, tok32), (VMEM, tok), (VMEM, tok)],
    )
    for layer in range(layers):
        (kq, pq), (ko, po) = fetched[layer, "a"]
        if layer:
            ln_t = over_x(ln_o)
        qkv_o, wqkv = call(
            qkv_body,
            "qkv",
            [(SMEM, pos), (VMEM, ln_o), (VMEM, head_shift(layer)), (HBM, qkv_weight)]
            + [(HBM, v) for v in pq],
            [(VMEM, qkv_s), (VMEM, shape((width, 3 * half)))],
            [SEMS((tiles,))],
            gemm * 3 * half,
            layer=layer,
            keys=kq,
            f=dg,
        )
        if layer + 1 < layers:
            fetched[layer + 1, "a"] = packs[layer + 1, "a"](qkv_o[:ROWS])
        qkv_t, probs_t, ctx_t, send, wout = call(
            attend_other_body,
            "attend_other",
            [
                (SMEM, pos),
                (VMEM, ln_t),
                (VMEM, wqkv),
                (VMEM, head_shift(layer)),
                (VMEM, qkv_o),
                (VMEM, mask),
                (HBM, out_weight),
            ]
            + [(HBM, v) for v in po],
            [(VMEM, s) for s in (qkv_s, probs_s, ctx_s, tok, shape((half, width)))],
            [kv_v, SEMS((1,))],
            gemm * 5 * half,
            layer=layer,
            keys=ko,
        )
        got = over_x(send)
        probs_o, ctx_o, part = call(
            attend_own_body,
            "attend_own",
            [(VMEM, v) for v in (qkv_o, qkv_t, mask, wout)],
            [(VMEM, s) for s in (probs_s, ctx_s, tok32)],
            [kv_v],
            gemm * 3 * half,
        )
        middle, mlp_o = call(
            norm_body,
            "norm",
            [
                (VMEM, v)
                for v in (stream, part, got, shift(layer, 3), gain(layer, 1), shift(layer, 4))
            ],
            [(VMEM, tok32), (VMEM, tok)],
        )
        mlp_t = over_x(mlp_o)
        if layer + 1 < layers:
            fetched[layer + 1, "m"] = packs[layer + 1, "m"](mlp_t[:ROWS])
        (k1, p1), (k2, p2) = fetched[layer, "m"]
        act1, slope_o, part, w1, w2 = call(
            mlp_own_body,
            "mlp_own",
            [
                (SMEM, pos),
                (VMEM, mlp_o),
                (VMEM, fc1_shift(layer)),
                (HBM, fc1_weight),
                (HBM, fc2_weight),
            ]
            + [(HBM, v) for v in p1]
            + [(HBM, v) for v in p2],
            [(VMEM, s) for s in (hid, hid, tok32, shape((width, ff)), shape((ff, width)))],
            [SEMS((tiles + 1,))],
            gemm * 2 * ff,
            layer=layer,
            keys1=k1,
            keys2=k2,
            f=ffg,
        )
        weights_v = [pltpu.VMEM((width, ff), BF16), pltpu.VMEM((ff, width), BF16), SEMS((tiles + 1,))]
        act2, slope_t, send = call(
            mlp_other_body,
            "mlp_other",
            [(VMEM, mlp_t), (VMEM, fc1_shift(layer)), (HBM, w1), (HBM, w2)],
            [(VMEM, s) for s in (hid, hid, tok)],
            weights_v,
            gemm * 2 * ff,
        )
        got = over_x(send)
        saved.append(
            dict(
                stream=stream,
                middle=middle,
                ln=(ln_o, ln_t),
                qkv=(qkv_o, qkv_t),
                probs=(probs_o, probs_t),
                ctx=(ctx_o, ctx_t),
                mlp=(mlp_o, mlp_t),
                act=(act1, act2),
                slope=(slope_o, slope_t),
                w=(wqkv, wout, w1, w2),
            )
        )
        if layer + 1 < layers:
            stream, ln_o = call(
                norm_body,
                "norm",
                [
                    (VMEM, v)
                    for v in (
                        middle,
                        part,
                        got,
                        shift(layer, 5),
                        gain(layer + 1, 0),
                        shift(layer + 1, 0),
                    )
                ],
                [(VMEM, tok32), (VMEM, tok)],
            )
        else:
            outputs = call(
                last_body,
                "last",
                [(VMEM, v) for v in (middle, part, got, shift(layer, 5))],
                [(VMEM, shape((n, width)))],
            )[0]

    g_o, g_sum = call(
        pad_grad_body,
        "first_grad",
        [(VMEM, cotangent.reshape(n, width))],
        [(VMEM, tok), (VMEM, shape((1, width), F32))],
    )
    grad = g_o
    yk = [None] * layers
    ak = [None] * layers
    smalls = [None] * layers
    sums_s = shape((3, width), F32)

    def row1(cols):
        return shape((1, cols), F32)

    for layer in reversed(range(layers)):
        s = saved[layer]
        wqkv, wout, w1, w2 = s["w"]
        g_t = over_x(g_o)

        def mlp_back(a, g, kind):
            return call(
                mlp_back_body,
                "mlp_back",
                [(VMEM, g), (VMEM, s["slope"][a]), (HBM, w2), (HBM, w1)],
                [(VMEM, hid), (VMEM, kind), (VMEM, row1(ff))],
                [weights_v[1], weights_v[0], weights_v[2]],
                gemm * 2 * ff,
            )

        dp_o, part, sum_o = mlp_back(0, g_o, tok32)
        dp_t, send, sum_t = mlp_back(1, g_t, tok)
        got = over_x(send)
        mg = (ys, 4 * dg, width)
        yk[layer] = call(
            mlp_grads_body,
            "mlp_grads",
            [(HBM, v) for v in (*s["act"], g_o, g_t, *s["mlp"], dp_o, dp_t)],
            [(VMEM, shape(mg[1:]))] * ys,
            [
                pltpu.VMEM((2 * npad, width), BF16),
                pltpu.VMEM((2 * npad, ff), BF16),
                pltpu.VMEM((2 * npad, ff), BF16),
                pltpu.VMEM((2 * npad, width), BF16),
                pltpu.VMEM(mg, BF16),
                pltpu.VMEM(mg, BF16),
                SEMS((4,)),
                SEMS((64,)),
                SEMS((64,)),
            ],
            gemm * 4 * ff,
            collective=0,
            ys=ys,
        )
        d_middle, ga_o, sums_b = call(
            norm_back_body,
            "norm_back",
            [(VMEM, v) for v in (part, got, s["middle"], gain(layer, 1), grad)],
            [(VMEM, tok32), (VMEM, tok), (VMEM, sums_s)],
        )
        ga_t = over_x(ga_o)
        d_q, d_kv = call(
            attend_back_own_body,
            "attend_back_own",
            [(VMEM, v) for v in (ga_o, wout, *s["qkv"], s["probs"][0])],
            [(VMEM, ctx_s), (VMEM, shape((2 * npad, 2 * half), F32))],
            [kv_v, pltpu.VMEM((npad, half), BF16)],
            gemm * 4 * half,
        )
        mixed_o, mixed_t, send, sum_q = call(
            attend_back_other_body,
            "attend_back_other",
            [(VMEM, v) for v in (ga_t, wout, *s["qkv"], s["probs"][1], d_q, d_kv, wqkv)],
            [(VMEM, qkv_s), (VMEM, qkv_s), (VMEM, tok), (VMEM, row1(3 * half))],
            [
                kv_v,
                pltpu.VMEM((npad, half), BF16),
                pltpu.VMEM((2 * npad, 2 * half), F32),
                pltpu.VMEM((npad, half), BF16),
            ],
            gemm * 7 * half,
        )
        got = over_x(send)
        ag = (ys, 2 * dg, width)
        part, *ak[layer] = call(
            attend_grads_body,
            "attend_grads",
            [(VMEM, mixed_o), (VMEM, wqkv)]
            + [(HBM, v) for v in (*s["ctx"], ga_o, ga_t, *s["ln"], mixed_o, mixed_t)],
            [(VMEM, tok32)] + [(VMEM, shape(ag[1:]))] * ys,
            [
                pltpu.VMEM((2 * npad, half), BF16),
                pltpu.VMEM((2 * npad, width), BF16),
                pltpu.VMEM((2 * npad, width), BF16),
                pltpu.VMEM((2 * npad, 3 * half), BF16),
                pltpu.VMEM(ag, BF16),
                pltpu.VMEM(ag, BF16),
                SEMS((4,)),
                SEMS((64,)),
                SEMS((64,)),
            ],
            gemm * 11 * half,
            collective=1,
            ys=ys,
        )
        grad, g_o, sums_a = call(
            norm_back_body,
            "norm_back",
            [(VMEM, v) for v in (part, got, s["stream"], gain(layer, 0), d_middle)],
            [(VMEM, tok32), (VMEM, tok), (VMEM, sums_s)],
        )
        plain = jnp.concatenate(
            [sums_a[:1], sums_b[:1], sums_a[1:2], sums_b[2:3], sums_b[1:2], g_sum]
        )
        plain = jnp.moveaxis(plain.reshape(6, group, dg), 1, 0)
        g_sum = sums_a[2:3]

        def place_heads(v, count=1):
            v = v.reshape(ys, 1, count, dg)
            out = jnp.where((lax.broadcasted_iota(jnp.int32, (1, 2, 1, 1), 1) == x), v, 0.0)
            return out.reshape(group, count, dg)

        smalls[layer] = jnp.concatenate(
            [
                plain,
                place_heads(sum_q[:, :half]),
                place_heads(sum_q[:, 2 * half :]),
                place_heads(sum_o + sum_t, many),
            ],
            axis=1,
        )
    input_grad = g_o[:n].reshape(activations.shape)

    def add_all(first, rest):
        total = first.astype(F32)
        for v in rest:
            total = total + v.astype(F32)
        return total.astype(BF16)

    z_groups = [[2 * i + c for i in range(zs)] for c in range(2)]
    done = []
    for layer in range(1, layers):
        m = add_all(yk[layer][0], [over_y(yk[layer][k], k) for k in range(1, ys)])
        a = add_all(ak[layer][0], [over_y(ak[layer][k], k) for k in range(1, ys)])
        m = lax.psum(m, "replica", axis_index_groups=z_groups)
        a = lax.psum(a, "replica", axis_index_groups=z_groups)
        done.append(jnp.concatenate([m, a], axis=0))
    mlp_got = [over_y(yk[0][k], k) for k in range(1, ys)]
    small_sum = jnp.concatenate(smalls, axis=1)
    totals, small_sum = tail(
        yk[0][0], mlp_got, ak[0], small_sum, done, ys=ys, zs=zs, dg=dg
    )
    outs = [
        shape((layers, dg, 2 * ff), F32),
        shape((layers, ffg, width), F32),
        shape((layers, dg, 3 * width), F32),
        shape((layers, dg, width), F32),
    ]
    fc1, fc2, qkv, out = call(
        place_body,
        "place",
        [(SMEM, pos)] + [(VMEM, v) for t in totals for v in t],
        [(VMEM, s) for s in outs],
        ys=ys,
    )
    small_sum = small_sum.reshape(layers, 8 + many, dg)
    order = [2, 6, 7, 3, 4, 5]
    grad_biases = jnp.stack([small_sum[:, i] for i in order], axis=1)
    return (
        outputs.reshape(activations.shape),
        input_grad,
        qkv,
        out,
        fc1,
        fc2,
        small_sum[:, :2],
        grad_biases,
        small_sum[:, 8:].reshape(layers, many * dg),
    )


def solution(mesh):
    tokens = P("group", "replica", None, None)
    rows = P(None, "group", None)
    last = P(None, None, "group")
    return jax.shard_map(
        shards,
        mesh=mesh,
        in_specs=(
            tokens,
            P("group", "replica", None),
            rows,
            rows,
            rows,
            rows,
            last,
            last,
            P(None, "group"),
            tokens,
        ),
        out_specs=(tokens, tokens, rows, rows, rows, rows, last, last, P(None, "group")),
        check_vma=False,
    )
```
